8 devices in a mesh: dp: 1 (over z), tp: 2 (over y), sp: 4 (over x, core).
Axes of the slice: x: 2, y: 2, z: 1, core: 2. Of those that a mesh axis runs over, the one named last changes fastest.
Arguments:
- hidden: bfloat16 [32, 5120], P('dp')
- norm_gain: float32 [5120], replicated
- w_query: bfloat16 [5120, 5120], P(None, 'tp')
- w_key: bfloat16 [5120, 5120], P(None, 'tp')
- w_value: bfloat16 [5120, 5120], P(None, 'tp')
- w_out: bfloat16 [5120, 5120], P('tp')
- k_cache: bfloat16 [32, 1024, 40, 128], P('dp', 'sp', 'tp')
- v_cache: bfloat16 [32, 1024, 40, 128], P('dp', 'sp', 'tp')
- positions: int32 [32], P('dp')
Outputs:
- output 1: bfloat16 [32, 5120], P('dp')
- output 2: bfloat16 [32, 1024, 40, 128], P('dp', 'sp', 'tp')
- output 3: bfloat16 [32, 1024, 40, 128], P('dp', 'sp', 'tp')
All inputs are finite; a program needn't handle non-finite values.
Results may differ from the reference program's by a relative error of at most 0.00274627.
Values sent between devices are 32-bit elements.
A program may use at most 1.25 GiB of HBM per device.

```python
import jax
import jax.numpy as jnp
from jax import lax

D = 5120
HEADS = 40
KV_HEADS = 40
HEAD = 128
BATCH = 32
SEQ = 1024
ROPE_BASE = 1000000
EPS = 1e-5
GROUP = HEADS // KV_HEADS


def rotary(tensor, positions):
    half_dim = tensor.shape[-1] // 2
    inv_freq = 1.0 / (ROPE_BASE ** (jnp.arange(half_dim, dtype=jnp.float32) * 2.0 / tensor.shape[-1]))
    angles = positions.astype(jnp.float32)[:, None, None] * inv_freq[None, None, :]
    cosine = jnp.cos(angles)
    sine_val = jnp.sin(angles)
    first_half = tensor[..., :half_dim]
    second_half = tensor[..., half_dim:]
    return jnp.concatenate([first_half * cosine - second_half * sine_val, first_half * sine_val + second_half * cosine], axis=-1)


def smooth_field(base_key, amplitude, noise_scale):
    key_coef, key_noise = jax.random.split(base_key)
    num_freq = 4
    seq_frac = jnp.arange(SEQ, dtype=jnp.float32) / SEQ
    freq_list = jnp.arange(1, num_freq + 1, dtype=jnp.float32)
    phases = 2.0 * jnp.pi * seq_frac[:, None] * freq_list[None, :]
    basis_mat = jnp.concatenate([jnp.cos(phases), jnp.sin(phases)], axis=1)
    coef_mat = jax.random.normal(key_coef, (BATCH, 2 * num_freq, KV_HEADS * HEAD), jnp.float32) * (amplitude / num_freq ** 0.5)
    smooth_part = jnp.einsum("sf,bfc->bsc", basis_mat, coef_mat)
    noise_part = jax.random.normal(key_noise, (BATCH, SEQ, KV_HEADS * HEAD), jnp.float32)
    return (smooth_part + noise_scale * noise_part).reshape(BATCH, SEQ, KV_HEADS, HEAD)


def draw_positions(base_key):
    key_len, key_pick = jax.random.split(base_key)
    pos_draw = jax.random.randint(key_len, (BATCH,), SEQ // 4, SEQ, jnp.int32)
    longest = jax.random.randint(key_pick, (), 0, BATCH, jnp.int32)
    return jnp.where(jnp.arange(BATCH) == longest, SEQ - 1, pos_draw).astype(jnp.int32)


def setup_inputs(seed: int = 0, part: int = 0) -> dict:
    key_list = jax.random.split(jax.random.key(seed), 9)
    q_width = HEADS * HEAD
    kv_width = KV_HEADS * HEAD
    norm_gain = 1.0 + 0.3 * jax.random.normal(key_list[0], (D,), jnp.float32)
    w_query32 = jax.random.normal(key_list[1], (D, q_width), jnp.float32) * D ** -0.5
    head_zero = w_query32.reshape(D, KV_HEADS, GROUP, HEAD)[:, :, 0, :].reshape(D, kv_width)
    w_key32 = 0.75 * head_zero + 0.66 * jax.random.normal(key_list[2], (D, kv_width), jnp.float32) * D ** -0.5
    w_value32 = jax.random.normal(key_list[3], (D, kv_width), jnp.float32) * D ** -0.5
    w_out32 = jax.random.normal(key_list[4], (q_width, D), jnp.float32) * q_width ** -0.5
    hidden = jax.random.normal(jax.random.fold_in(key_list[5], part), (BATCH, D), jnp.float32)
    k_cache = smooth_field(jax.random.fold_in(key_list[6], part), 1.2, 0.5)
    v_cache = smooth_field(jax.random.fold_in(key_list[7], part), 1.5, 0.5)
    positions = draw_positions(jax.random.fold_in(key_list[8], part))
    return {
        "hidden": hidden.astype(jnp.bfloat16),
        "norm_gain": norm_gain,
        "w_query": w_query32.astype(jnp.bfloat16),
        "w_key": w_key32.astype(jnp.bfloat16),
        "w_value": w_value32.astype(jnp.bfloat16),
        "w_out": w_out32.astype(jnp.bfloat16),
        "k_cache": k_cache.astype(jnp.bfloat16),
        "v_cache": v_cache.astype(jnp.bfloat16),
        "positions": positions,
    }


def reference(hidden, norm_gain, w_query, w_key, w_value, w_out, k_cache, v_cache, positions):
    resid_f32 = hidden.astype(jnp.float32)
    normed = (resid_f32 * lax.rsqrt(jnp.mean(resid_f32 * resid_f32, axis=-1, keepdims=True) + EPS) * norm_gain).astype(jnp.bfloat16)
    q_proj = jnp.dot(normed, w_query, preferred_element_type=jnp.float32).reshape(BATCH, HEADS, HEAD)
    k_proj = jnp.dot(normed, w_key, preferred_element_type=jnp.float32).reshape(BATCH, KV_HEADS, HEAD)
    v_new = jnp.dot(normed, w_value, preferred_element_type=jnp.float32).astype(jnp.bfloat16).reshape(BATCH, KV_HEADS, HEAD)
    q_rot = rotary(q_proj, positions).astype(jnp.bfloat16).reshape(BATCH, KV_HEADS, GROUP, HEAD)
    k_new = rotary(k_proj, positions).astype(jnp.bfloat16)
    slot_mask = (jnp.arange(SEQ)[None, :] == positions[:, None])[:, :, None, None]
    k_updated = jnp.where(slot_mask, k_new[:, None], k_cache)
    v_updated = jnp.where(slot_mask, v_new[:, None], v_cache)
    score_scale = HEAD ** -0.5

    def one_sequence(seq_args):
        q_seq, k_seq, v_seq, last_pos = seq_args
        scores = jnp.einsum("kgd,skd->kgs", q_seq.astype(jnp.float32), k_seq.astype(jnp.float32)) * score_scale
        scores = jnp.where(jnp.arange(SEQ) <= last_pos, scores, -jnp.inf)
        attn_prob = jax.nn.softmax(scores, axis=-1)
        return jnp.einsum("kgs,skd->kgd", attn_prob, v_seq.astype(jnp.float32))

    attn_out = lax.map(one_sequence, (q_rot, k_updated, v_updated, positions))
    attn_out = attn_out.astype(jnp.bfloat16).reshape(BATCH, HEADS * HEAD)
    proj_out = jnp.dot(attn_out, w_out, preferred_element_type=jnp.float32)
    return (resid_f32 + proj_out).astype(jnp.bfloat16), k_updated, v_updated
```

```python
import jax
import jax.numpy as jnp
import numpy as np
from jax import lax
from jax.experimental import pallas as pl
from jax.experimental.pallas import tpu as pltpu
from jax.sharding import PartitionSpec as P

ROPE_BASE = 1000000.0
EPS = 1e-5
NEG_BIG = -1e30
MESH = pl.DeviceIdType.MESH
ANY = pl.BlockSpec(memory_space=pl.ANY)
VMEM = pl.BlockSpec(memory_space=pltpu.VMEM)
SMEM = pl.BlockSpec(memory_space=pltpu.SMEM)

B = 32
D = 5120
HL = 20
HD = 128
SL = 256
HS = 5
CW = HS * HD
KC = 512
NKC = D // KC
OC = 1280
OCH = 256
NOC = OC // OCH
SLOTS = 12
AHEAD = 8


def peers():
    sp = lax.axis_index("sp")
    across = lax.rem(sp + 2, 4)
    core = sp + 1 - 2 * lax.rem(sp, 2)
    return sp, across, core


def remote(src, dst, send, recv, dev):
    return pltpu.make_async_remote_copy(src_ref=src, dst_ref=dst, send_sem=send, recv_sem=recv,
                                        device_id=dev, device_id_type=MESH)


def qkv_kernel(pos_ref, h_ref, gain_ref, freq_ref, wq_ref, wk_ref, wv_ref, out_ref,
               wbuf, xn, g, wsem, ssem, rsem):
    sp, across, core = peers()
    bar = pltpu.get_barrier_semaphore()
    for dev in (across, core):
        pl.semaphore_signal(bar, inc=1, device_id={"sp": dev}, device_id_type=MESH)
    cols = pl.ds(pl.multiple_of(sp * CW, HD), CW)

    def chunk_copy(kind, c):
        src = (wq_ref, wk_ref, wv_ref)[kind]
        rows = pl.ds(pl.multiple_of(c * KC, KC), KC)
        return pltpu.make_async_copy(src.at[rows, cols], wbuf.at[kind, rows], wsem.at[kind, c])

    for kind in range(3):
        for c in range(NKC):
            chunk_copy(kind, c).start()

    x = h_ref[...].astype(jnp.float32)
    inv = lax.rsqrt(jnp.mean(x * x, axis=-1, keepdims=True) + EPS)
    xn[...] = (x * inv * gain_ref[...]).astype(jnp.bfloat16)
    row = lax.broadcasted_iota(jnp.int32, (B, HD), 0)
    lane = lax.broadcasted_iota(jnp.int32, (B, HD), 1)
    pos = jnp.zeros((B, HD), jnp.int32)
    for b in range(B):
        pos = jnp.where(row == b, pos_ref[b], pos)
    angles = pos.astype(jnp.float32) * freq_ref[...]
    cosine = jnp.cos(angles)
    sine = jnp.sin(angles)
    sine = jnp.where(lane < HD // 2, -sine, sine)
    pl.semaphore_wait(bar, 2)

    own = pl.ds(pl.multiple_of(sp * HS * B, B), HS * B)
    far = pl.ds(pl.multiple_of(across * HS * B, B), HS * B)

    def copies(kind):
        return (remote(g.at[kind, own], g.at[kind, own], ssem.at[kind, 0], rsem.at[kind, 0], {"sp": across}),
                remote(g.at[kind, own], g.at[kind, own], ssem.at[kind, 1], rsem.at[kind, 1], {"sp": core}),
                remote(g.at[kind, far], g.at[kind, far], ssem.at[kind, 2], rsem.at[kind, 2], {"sp": core}))

    for kind in range(3):
        def body(c, acc):
            chunk_copy(kind, c).wait()
            rows = pl.ds(pl.multiple_of(c * KC, KC), KC)
            return acc + jnp.dot(xn[:, rows], wbuf[kind, rows, :], preferred_element_type=jnp.float32)
        acc = lax.fori_loop(0, NKC, body, jnp.zeros((B, CW), jnp.float32))
        for i in range(HS):
            u = acc[:, i * HD:(i + 1) * HD]
            if kind < 2:
                u = u * cosine + pltpu.roll(u, HD // 2, 1) * sine
            g[kind, pl.ds(pl.multiple_of(sp * HS * B + i * B, B), B), :] = u.astype(jnp.bfloat16).astype(jnp.float32)
        first, second, _ = copies(kind)
        first.start()
        second.start()
        if kind > 0:
            prev = copies(kind - 1)
            prev[0].wait_recv()
            prev[2].start()
    last = copies(2)
    last[0].wait_recv()
    last[2].start()
    for kind in range(3):
        for i, c in enumerate(copies(kind)):
            if i == 0:
                c.wait_send()
            else:
                c.wait()
    out_ref[...] = g[...]


def cache_kernel(pos_ref, g_ref, k_ref, v_ref, ko_ref, vo_ref, acc_ref, ml_ref,
                 kbuf, vbuf, sbuf, rsem, wsem):
    base = lax.axis_index("sp") * SL

    def reads(b):
        slot = lax.rem(b, SLOTS)
        return (pltpu.make_async_copy(k_ref.at[b], kbuf.at[slot], rsem.at[0, slot]),
                pltpu.make_async_copy(v_ref.at[b], vbuf.at[slot], rsem.at[1, slot]))

    def writes(b):
        slot = lax.rem(b, SLOTS)
        return (pltpu.make_async_copy(kbuf.at[slot], ko_ref.at[b], wsem.at[0, slot]),
                pltpu.make_async_copy(vbuf.at[slot], vo_ref.at[b], wsem.at[1, slot]))

    for b in range(AHEAD):
        for c in reads(b):
            c.start()
    ml_ref[...] = jnp.zeros_like(ml_ref)

    def arrive(b):
        slot = lax.rem(b, SLOTS)
        for c in reads(b):
            c.wait()
        at = pos_ref[b] - base

        @pl.when((at >= 0) & (at < SL))
        def _():
            start = pl.multiple_of((at // 16) * 16, 16)
            hit = lax.broadcasted_iota(jnp.int32, (16, HD), 0) == at - start
            for kind, buf in ((1, kbuf), (2, vbuf)):
                for h in range(HL):
                    new = jnp.broadcast_to(g_ref[kind, pl.ds(h * B + b, 1), :], (16, HD))
                    old = buf[slot, h, pl.ds(start, 16), :].astype(jnp.float32)
                    buf[slot, h, pl.ds(start, 16), :] = jnp.where(hit, new, old).astype(jnp.bfloat16)

    qrow = lax.broadcasted_iota(jnp.int32, (HL, HD), 0)
    prow = lax.broadcasted_iota(jnp.int32, (HL, SL), 0)
    pcol = lax.broadcasted_iota(jnp.int32, (HL, SL), 1)
    mlane = lax.broadcasted_iota(jnp.int32, (HL, HD), 1)

    def score(b):
        slot = lax.rem(b, SLOTS)
        q = g_ref[0, pl.ds(b, HL, stride=B), :]
        s = jnp.zeros((HL, SL), jnp.float32)
        for h in range(HL):
            qh = jnp.where(qrow == h, q, 0.0).astype(jnp.bfloat16)
            s = s + lax.dot_general(qh, kbuf[slot, h], (((1,), (1,)), ((), ())), preferred_element_type=jnp.float32)
        sbuf[lax.rem(b, 2)] = s * (HD ** -0.5)

    def value(b):
        slot = lax.rem(b, SLOTS)
        valid = pcol <= pos_ref[b] - base
        s = jnp.where(valid, sbuf[lax.rem(b, 2)], NEG_BIG)
        m = jnp.max(s, axis=-1, keepdims=True)
        p = jnp.where(valid, jnp.exp(s - m), 0.0)
        total = jnp.sum(p, axis=-1, keepdims=True)
        o = jnp.zeros((HL, HD), jnp.float32)
        for h in range(HL):
            ph = jnp.where(prow == h, p, 0.0).astype(jnp.bfloat16)
            o = o + jnp.dot(ph, vbuf[slot, h], preferred_element_type=jnp.float32)
        acc_ref[pl.ds(b, HL, stride=B), :] = o
        ml_ref[...] = jnp.where(mlane == b, m, jnp.where(mlane == b + B, total, ml_ref[...]))

    def ahead(b):
        @pl.when(b + AHEAD < B)
        def _():
            @pl.when(b + AHEAD >= SLOTS)
            def _():
                for c in writes(b + AHEAD - SLOTS):
                    c.wait()
            for c in reads(b + AHEAD):
                c.start()

    arrive(0)
    ahead(0)
    score(0)
    writes(0)[0].start()

    @pl.loop(1, B)
    def _(b):
        arrive(b)
        ahead(b)
        score(b)
        value(b - 1)
        writes(b)[0].start()
        writes(b - 1)[1].start()

    value(B - 1)
    writes(B - 1)[1].start()
    for b in range(B - SLOTS, B):
        for c in writes(b):
            c.wait()


def out_kernel(acc_ref, ml_ref, h_ref, w_ref, out_ref,
               wbuf, mlbuf, send1, r1, pair, r2, oall, ypart, yin, yall,
               wsem, mlsend, mlrecv, ssem, rsem, ysend, yrecv):
    sp, across, core = peers()
    diag = 3 - sp
    tp = lax.axis_index("tp")
    c01 = lax.rem(sp, 2)
    bar = pltpu.get_barrier_semaphore()
    half = HL // 2
    hr = half * B

    wcopies = [pltpu.make_async_copy(w_ref.at[pl.ds(i * KC, KC), pl.ds(pl.multiple_of(sp * OC, HD), OC)],
                                     wbuf.at[pl.ds(i * KC, KC)], wsem.at[i]) for i in range(HL * HD // KC)]
    for c in wcopies:
        c.start()
    for dev in (across, core, diag):
        pl.semaphore_signal(bar, inc=1, device_id={"sp": dev}, device_id_type=MESH)
    pl.semaphore_signal(bar, inc=1, device_id={"tp": 1 - tp}, device_id_type=MESH)
    mlbuf[0] = ml_ref[...]
    send1[...] = acc_ref[pl.ds(pl.multiple_of((1 - c01) * hr, B), hr), :]
    pl.semaphore_wait(bar, 4)

    mlc = [remote(mlbuf.at[0], mlbuf.at[i + 1], mlsend.at[i], mlrecv.at[i], {"sp": dev})
           for i, dev in enumerate((core, across, diag))]
    c1 = remote(send1, r1, ssem.at[0], rsem.at[0], {"sp": core})
    mlc[0].start()
    c1.start()
    mlc[1].start()
    mlc[2].start()

    def columns(table):
        t = jnp.where(c01 == 0, table[:half], table[half:])
        t = jnp.concatenate([t, jnp.zeros((HD - half, HD), jnp.float32)], axis=0)
        return jnp.transpose(t)

    mlc[0].wait_recv()
    own = mlbuf[0]
    other = mlbuf[1]
    m_pair = jnp.maximum(own, other)
    f_own = columns(jnp.exp(own - m_pair))
    f_other = columns(jnp.exp(other - m_pair))
    c1.wait_recv()
    for i in range(half):
        mine = acc_ref[pl.ds(pl.multiple_of(c01 * hr + i * B, B), B), :]
        theirs = r1[i * B:(i + 1) * B, :]
        pair[i * B:(i + 1) * B, :] = mine * f_own[:B, i:i + 1] + theirs * f_other[:B, i:i + 1]
    c2 = remote(pair, r2, ssem.at[1], rsem.at[1], {"sp": across})
    c2.start()

    mlc[1].wait_recv()
    mlc[2].wait_recv()
    tabs = [mlbuf[i] for i in range(4)]
    m_far = jnp.maximum(tabs[2], tabs[3])
    m_all = jnp.maximum(m_pair, m_far)
    total = jnp.zeros((HL, HD), jnp.float32)
    for t in tabs:
        total = total + jnp.exp(t - m_all) * pltpu.roll(t, HD - B, 1)
    lane = lax.broadcasted_iota(jnp.int32, (HL, HD), 1)
    total = jnp.where(lane < B, total, 1.0)
    g_pair = columns(jnp.exp(m_pair - m_all) / total)
    g_far = columns(jnp.exp(m_far - m_all) / total)
    c2.wait_recv()
    for i in range(half):
        o = pair[i * B:(i + 1) * B, :] * g_pair[:B, i:i + 1] + r2[i * B:(i + 1) * B, :] * g_far[:B, i:i + 1]
        oall[pl.ds(pl.multiple_of(c01 * hr + i * B, B), B), :] = o
    mine = pl.ds(pl.multiple_of(c01 * hr, B), hr)
    c3 = remote(oall.at[mine], oall.at[mine], ssem.at[2], rsem.at[2], {"sp": core})
    c3.start()
    for c in wcopies:
        c.wait()
    c3.wait_recv()

    lhs = [jnp.concatenate([oall[(2 * i) * B:(2 * i + 1) * B, :], oall[(2 * i + 1) * B:(2 * i + 2) * B, :]],
                           axis=1).astype(jnp.bfloat16) for i in range(half)]

    def piece(j):
        return (remote(ypart.at[j], yin.at[j], ysend.at[0, j], yrecv.at[0, j], {"tp": 1 - tp}),
                remote(yall.at[sp, j], yall.at[sp, j], ysend.at[1, j], yrecv.at[1, j], {"sp": across}),
                remote(yall.at[sp, j], yall.at[sp, j], ysend.at[2, j], yrecv.at[2, j], {"sp": core}),
                remote(yall.at[across, j], yall.at[across, j], ysend.at[3, j], yrecv.at[3, j], {"sp": core}))

    for j in range(NOC):
        y = jnp.zeros((B, OCH), jnp.float32)
        for i in range(half):
            y = y + jnp.dot(lhs[i], wbuf[i * 2 * HD:(i + 1) * 2 * HD, j * OCH:(j + 1) * OCH],
                            preferred_element_type=jnp.float32)
        ypart[j] = y
        piece(j)[0].start()
    for j in range(NOC):
        p = piece(j)
        p[0].wait_recv()
        yall[sp, j] = ypart[j] + yin[j]
        p[1].start()
        p[2].start()
    for j in range(NOC):
        p = piece(j)
        p[1].wait_recv()
        p[3].start()
    for j in range(NOC):
        p = piece(j)
        p[2].wait_recv()
        p[3].wait_recv()
        for i in range(4):
            p[i].wait_send()
    for s in range(4):
        for j in range(NOC):
            at = s * OC + j * OCH
            out_ref[:, at:at + OCH] = (h_ref[:, at:at + OCH].astype(jnp.float32) + yall[s, j]).astype(jnp.bfloat16)
    for c in (c1, c2, c3, *mlc):
        c.wait_send()


def solution(mesh):
    half_dim = HD // 2
    freq = 1.0 / (ROPE_BASE ** (np.arange(half_dim, dtype=np.float64) * 2.0 / HD))
    freq = np.concatenate([freq, freq]).astype(np.float32)[None, :]

    def local_step(hidden, norm_gain, w_query, w_key, w_value, w_out, k_cache, v_cache, positions):
        f32, bf16 = jnp.float32, jnp.bfloat16
        dma = pltpu.SemaphoreType.DMA
        g = pl.pallas_call(
            qkv_kernel,
            out_shape=jax.ShapeDtypeStruct((3, HL * B, HD), f32),
            in_specs=[SMEM, VMEM, VMEM, VMEM, ANY, ANY, ANY],
            out_specs=VMEM,
            scratch_shapes=[pltpu.VMEM((3, D, CW), bf16), pltpu.VMEM((B, D), bf16), pltpu.VMEM((3, HL * B, HD), f32),
                            dma((3, NKC)), dma((3, 3)), dma((3, 3))],
            compiler_params=pltpu.CompilerParams(collective_id=0, has_side_effects=True, vmem_limit_bytes=40 << 20),
            name="qkv",
        )(positions, hidden, norm_gain[None, :], jnp.asarray(freq), w_query, w_key, w_value)

        kt = jnp.transpose(k_cache, (0, 2, 1, 3))
        vt = jnp.transpose(v_cache, (0, 2, 1, 3))
        ko, vo, acc, ml = pl.pallas_call(
            cache_kernel,
            out_shape=(jax.ShapeDtypeStruct(kt.shape, bf16), jax.ShapeDtypeStruct(vt.shape, bf16),
                       jax.ShapeDtypeStruct((HL * B, HD), f32), jax.ShapeDtypeStruct((HL, HD), f32)),
            in_specs=[SMEM, VMEM, ANY, ANY],
            out_specs=(ANY, ANY, VMEM, VMEM),
            scratch_shapes=[pltpu.VMEM((SLOTS, HL, SL, HD), bf16), pltpu.VMEM((SLOTS, HL, SL, HD), bf16),
                            pltpu.VMEM((2, HL, SL), f32), dma((2, SLOTS)), dma((2, SLOTS))],
            compiler_params=pltpu.CompilerParams(vmem_limit_bytes=48 << 20),
            name="cache",
        )(positions, g, kt, vt)

        hr = HL // 2 * B
        out = pl.pallas_call(
            out_kernel,
            out_shape=jax.ShapeDtypeStruct((B, D), bf16),
            in_specs=[VMEM, VMEM, VMEM, ANY],
            out_specs=VMEM,
            scratch_shapes=[pltpu.VMEM((HL * HD, OC), bf16), pltpu.VMEM((4, HL, HD), f32),
                            pltpu.VMEM((hr, HD), f32), pltpu.VMEM((hr, HD), f32), pltpu.VMEM((hr, HD), f32),
                            pltpu.VMEM((hr, HD), f32), pltpu.VMEM((HL * B, HD), f32),
                            pltpu.VMEM((NOC, B, OCH), f32), pltpu.VMEM((NOC, B, OCH), f32),
                            pltpu.VMEM((4, NOC, B, OCH), f32),
                            dma((HL * HD // KC,)), dma((3,)), dma((3,)), dma((3,)), dma((3,)),
                            dma((4, NOC)), dma((4, NOC))],
            compiler_params=pltpu.CompilerParams(collective_id=1, has_side_effects=True, vmem_limit_bytes=32 << 20),
            name="out",
        )(acc, ml, hidden, w_out)
        return out, jnp.transpose(ko, (0, 2, 1, 3)), jnp.transpose(vo, (0, 2, 1, 3))

    cache_spec = P("dp", "sp", "tp", None)
    specs_in = (P("dp", None), P(None), P(None, "tp"), P(None, "tp"), P(None, "tp"), P("tp", None), cache_spec, cache_spec, P("dp"))
    specs_out = (P("dp", None), cache_spec, cache_spec)
    return jax.shard_map(local_step, mesh=mesh, in_specs=specs_in, out_specs=specs_out, check_vma=False)
```

```python
import jax
import jax.numpy as jnp
import numpy as np
from jax import lax
from jax.experimental import pallas as pl
from jax.experimental.pallas import tpu as pltpu
from jax.sharding import PartitionSpec as P

ROPE_BASE = 1000000.0
EPS = 1e-5
NEG_BIG = -1e30
MESH = pl.DeviceIdType.MESH
VMEM = pl.BlockSpec(memory_space=pltpu.VMEM)
SMEM = pl.BlockSpec(memory_space=pltpu.SMEM)

B = 32
D = 5120
HL = 20
HD = 128
SL = 256
HS = 5
CW = HS * HD
KC = 1280
NKC = D // KC
OC = 1280
OCH = 256
NOC = OC // OCH
OK = 512
NB = 8
NA = B - NB
SLOTS = 9
EARLY = 8
AHEAD = 5
SCALE = HD ** -0.5
HBM = pl.BlockSpec(memory_space=pltpu.HBM)


def peers():
    sp = lax.axis_index("sp")
    across = lax.rem(sp + 2, 4)
    core = sp + 1 - 2 * lax.rem(sp, 2)
    return sp, across, core


def remote(src, dst, send, recv, dev):
    return pltpu.make_async_remote_copy(src_ref=src, dst_ref=dst, send_sem=send, recv_sem=recv,
                                        device_id=dev, device_id_type=MESH)


def qkv_kernel(pos_hbm, h_hbm, gain_hbm, freq_hbm, wq_ref, wk_ref, wv_ref, k_ref, v_ref, out_ref, kring, vring,
               wbuf, xn, g, pos_ref, h_ref, gain_ref, freq_ref, insem, wsem, ssem, rsem, tsem):
    sp, across, core = peers()
    bar = pltpu.get_barrier_semaphore()
    for dev in (across, core):
        pl.semaphore_signal(bar, inc=1, device_id={"sp": dev}, device_id_type=MESH)
    cols = pl.ds(pl.multiple_of(sp * CW, HD), CW)
    small = [pltpu.make_async_copy(src, dst, insem.at[i]) for i, (src, dst) in enumerate(
        ((h_hbm, h_ref), (gain_hbm, gain_ref), (freq_hbm, freq_ref), (pos_hbm, pos_ref)))]
    for c in small:
        c.start()

    def chunk(kind, c):
        src = (wq_ref, wk_ref, wv_ref)[kind]
        rows = pl.ds(c * KC, KC)
        return pltpu.make_async_copy(src.at[rows, cols], wbuf.at[kind, rows], wsem.at[kind, c])

    chunks = [[chunk(kind, c) for c in range(NKC)] for kind in range(3)]
    for kind in range(3):
        for c in chunks[kind]:
            c.start()
    tiles = [pltpu.make_async_copy(src.at[b], dst.at[b], tsem.at[i, b])
             for b in range(EARLY) for i, (src, dst) in enumerate(((k_ref, kring), (v_ref, vring)))]

    for c in small:
        c.wait()
    x = h_ref[...].astype(jnp.float32)
    inv = lax.rsqrt(jnp.mean(x * x, axis=-1, keepdims=True) + EPS)
    xn[...] = (x * inv * gain_ref[...]).astype(jnp.bfloat16)
    row = lax.broadcasted_iota(jnp.int32, (B, HD), 0)
    lane = lax.broadcasted_iota(jnp.int32, (B, HD), 1)
    pos = jnp.zeros((B, HD), jnp.int32)
    for b in range(B):
        pos = jnp.where(row == b, pos_ref[b], pos)
    angles = pos.astype(jnp.float32) * freq_ref[...]
    cosine = jnp.cos(angles)
    sine = jnp.sin(angles)
    sine = jnp.where(lane < HD // 2, -sine, sine)
    pl.semaphore_wait(bar, 2)

    own = pl.ds(pl.multiple_of(sp * HS * B, B), HS * B)
    far = pl.ds(pl.multiple_of(across * HS * B, B), HS * B)
    links = [(remote(g.at[kind, own], g.at[kind, own], ssem.at[kind, 0], rsem.at[kind, 0], {"sp": across}),
              remote(g.at[kind, own], g.at[kind, own], ssem.at[kind, 1], rsem.at[kind, 1], {"sp": core}),
              remote(g.at[kind, far], g.at[kind, far], ssem.at[kind, 2], rsem.at[kind, 2], {"sp": core}))
             for kind in range(3)]

    for kind in range(3):
        acc = jnp.zeros((B, CW), jnp.float32)
        for c in range(NKC):
            chunks[kind][c].wait()
            rows = slice(c * KC, (c + 1) * KC)
            acc = acc + jnp.dot(xn[:, rows], wbuf[kind, rows, :], preferred_element_type=jnp.float32)
        for i in range(HS):
            u = acc[:, i * HD:(i + 1) * HD]
            if kind < 2:
                u = u * cosine + pltpu.roll(u, HD // 2, 1) * sine
            g[kind, pl.ds(pl.multiple_of(sp * HS * B + i * B, B), B), :] = u.astype(jnp.bfloat16).astype(jnp.float32)
        links[kind][0].start()
        links[kind][1].start()
        if kind > 0:
            links[kind - 1][0].wait_recv()
            links[kind - 1][2].start()
        if kind == 1:
            for c in tiles:
                c.start()
    links[2][0].wait_recv()
    links[2][2].start()
    for kind in range(3):
        links[kind][0].wait_send()
        links[kind][1].wait()
        links[kind][2].wait()
    out_ref[...] = g[...]
    for c in tiles:
        c.wait()


def row_of(rows, h, x):
    return jnp.where(rows == h, x, 0.0).astype(jnp.bfloat16)


def scores(q, keys):
    rows = lax.broadcasted_iota(jnp.int32, (HL, HD), 0)
    s = jnp.zeros((HL, SL), jnp.float32)
    for h in range(HL):
        s = s + lax.dot_general(row_of(rows, h, q), keys(h), (((1,), (1,)), ((), ())), preferred_element_type=jnp.float32)
    return s * SCALE


def weighted(p, values):
    rows = lax.broadcasted_iota(jnp.int32, (HL, SL), 0)
    o = jnp.zeros((HL, HD), jnp.float32)
    for h in range(HL):
        o = o + jnp.dot(row_of(rows, h, p), values(h), preferred_element_type=jnp.float32)
    return o


def insert_row(g_ref, b, at, tile_refs):
    @pl.when((at >= 0) & (at < SL))
    def _():
        start = pl.multiple_of((at // 16) * 16, 16)
        hit = lax.broadcasted_iota(jnp.int32, (16, HD), 0) == at - start
        for kind, buf, slot in tile_refs:
            for h in range(HL):
                new = jnp.broadcast_to(g_ref[kind, pl.ds(h * B + b, 1), :], (16, HD))
                old = buf[slot, h, pl.ds(start, 16), :].astype(jnp.float32)
                buf[slot, h, pl.ds(start, 16), :] = jnp.where(hit, new, old).astype(jnp.bfloat16)


def put_stats(ml_ref, b, m, total):
    lane = lax.broadcasted_iota(jnp.int32, (HL, HD), 1)
    ml_ref[...] = jnp.where(lane == b, m, jnp.where(lane == b + B, total, ml_ref[...]))


def cache_kernel(pos_ref, g_ref, k_ref, v_ref, kin, vin, ko_ref, vo_ref, acc_ref, ml_ref, kbuf, vbuf,
                 sbuf, rsem, wsem):
    del kin, vin
    base = lax.axis_index("sp") * SL

    def reads(b):
        slot = lax.rem(b, SLOTS)
        return (pltpu.make_async_copy(k_ref.at[b], kbuf.at[slot], rsem.at[0, slot]),
                pltpu.make_async_copy(v_ref.at[b], vbuf.at[slot], rsem.at[1, slot]))

    def write_k(b):
        slot = lax.rem(b, SLOTS)
        return pltpu.make_async_copy(kbuf.at[slot], ko_ref.at[b], wsem.at[0, slot])

    def write_v(b):
        slot = lax.rem(b, SLOTS)
        return pltpu.make_async_copy(vbuf.at[slot], vo_ref.at[b], wsem.at[1, slot])

    for b in range(EARLY, SLOTS):
        for c in reads(b):
            c.start()
    ml_ref[...] = jnp.zeros_like(ml_ref)

    def arrive(b):
        @pl.when(b >= EARLY)
        def _():
            for c in reads(b):
                c.wait()
        slot = lax.rem(b, SLOTS)
        insert_row(g_ref, b, pos_ref[b] - base, ((1, kbuf, slot), (2, vbuf, slot)))

    pcol = lax.broadcasted_iota(jnp.int32, (HL, SL), 1)

    def score(b):
        slot = lax.rem(b, SLOTS)
        sbuf[lax.rem(b, 2)] = scores(g_ref[0, pl.ds(b, HL, stride=B), :], lambda h: kbuf[slot, h])

    def value(b):
        slot = lax.rem(b, SLOTS)
        valid = pcol <= pos_ref[b] - base
        s = jnp.where(valid, sbuf[lax.rem(b, 2)], NEG_BIG)
        m = jnp.max(s, axis=-1, keepdims=True)
        p = jnp.where(valid, jnp.exp(s - m), 0.0)
        total = jnp.sum(p, axis=-1, keepdims=True)
        acc_ref[pl.ds(b, HL, stride=NA), :] = weighted(p, lambda h: vbuf[slot, h])
        put_stats(ml_ref, b, m, total)

    def ahead(b):
        @pl.when((b + AHEAD >= SLOTS) & (b + AHEAD < NA))
        def _():
            write_k(b + AHEAD - SLOTS).wait()
            write_v(b + AHEAD - SLOTS).wait()
            for c in reads(b + AHEAD):
                c.start()

    arrive(0)
    ahead(0)
    score(0)
    write_k(0).start()

    @pl.loop(1, NA)
    def _(b):
        arrive(b)
        ahead(b)
        score(b)
        value(b - 1)
        write_k(b).start()
        write_v(b - 1).start()

    value(NA - 1)
    write_v(NA - 1).start()
    for b in range(NA - SLOTS, NA):
        write_k(b).wait()
        write_v(b).wait()


def tail_kernel(pos_ref, g_ref, acc_a, ml_a, h_ref, k_ref, v_ref, w_ref, out_ref, kt, vt,
                wbuf, sbuf, acc_b, ml_b, *scratch):
    sp, across, core = peers()
    diag = 3 - sp
    tp = lax.axis_index("tp")
    c01 = lax.rem(sp, 2)
    base = sp * SL
    half = HL // 2
    rsem, wsem = scratch[:2]
    bar = pltpu.get_barrier_semaphore()
    for dev in (across, core, diag):
        pl.semaphore_signal(bar, inc=1, device_id={"sp": dev}, device_id_type=MESH)
    pl.semaphore_signal(bar, inc=1, device_id={"tp": 1 - tp}, device_id_type=MESH)

    def reads(t):
        return (pltpu.make_async_copy(k_ref.at[NA + t], kt.at[t], rsem.at[0, t]),
                pltpu.make_async_copy(v_ref.at[NA + t], vt.at[t], rsem.at[1, t]))

    for t in range(NB):
        for c in reads(t):
            c.start()
    wcopies = [pltpu.make_async_copy(w_ref.at[pl.ds(i * OK, OK), pl.ds(pl.multiple_of(sp * OC, HD), OC)],
                                     wbuf.at[pl.ds(i * OK, OK)], wsem.at[i]) for i in range(HL * HD // OK)]
    for c in wcopies:
        c.start()

    def columns(table):
        t = jnp.where(c01 == 0, table[:half], table[half:])
        t = jnp.concatenate([t, jnp.zeros((HD - half, HD), jnp.float32)], axis=0)
        return jnp.transpose(t)

    class Rows:
        def __init__(self, n, first, acc, ml, bufs):
            self.n, self.first, self.acc, self.ml = n, first, acc, ml
            (self.mlbuf, self.r1, self.pair, self.r2, self.oall, self.ypart, self.yin, self.yall,
             mls, mlr, s, r, ys, yr) = bufs
            hr = half * n
            mine = pl.ds(pl.multiple_of(c01 * hr, 8), hr)
            theirs = pl.ds(pl.multiple_of((1 - c01) * hr, 8), hr)
            self.mlc = [remote(self.mlbuf.at[0], self.mlbuf.at[i + 1], mls.at[i], mlr.at[i], {"sp": dev})
                        for i, dev in enumerate((core, across, diag))]
            self.c1 = remote(acc.at[theirs], self.r1, s.at[0], r.at[0], {"sp": core})
            self.c2 = remote(self.pair, self.r2, s.at[1], r.at[1], {"sp": across})
            self.c3 = remote(self.oall.at[mine], self.oall.at[mine], s.at[2], r.at[2], {"sp": core})
            ya = self.yall
            self.pieces = [(remote(self.ypart.at[j], self.yin.at[j], ys.at[0, j], yr.at[0, j], {"tp": 1 - tp}),
                            remote(ya.at[sp, j], ya.at[sp, j], ys.at[1, j], yr.at[1, j], {"sp": across}),
                            remote(ya.at[sp, j], ya.at[sp, j], ys.at[2, j], yr.at[2, j], {"sp": core}),
                            remote(ya.at[across, j], ya.at[across, j], ys.at[3, j], yr.at[3, j], {"sp": core}))
                           for j in range(NOC)]

        def mine(self, i):
            return pl.ds(pl.multiple_of((c01 * half + i) * self.n, 8), self.n)

        def start(self):
            self.mlbuf[0] = self.ml[...]
            self.mlc[0].start()
            self.c1.start()
            self.mlc[1].start()
            self.mlc[2].start()

        def merge_core(self):
            n = self.n
            self.mlc[0].wait_recv()
            own, other = self.mlbuf[0], self.mlbuf[1]
            m_pair = jnp.maximum(own, other)
            f_own, f_other = columns(jnp.exp(own - m_pair)), columns(jnp.exp(other - m_pair))
            self.c1.wait_recv()
            for i in range(half):
                rows = slice(i * n, (i + 1) * n)
                self.pair[rows, :] = (self.acc[self.mine(i), :] * f_own[self.first:self.first + n, i:i + 1]
                                      + self.r1[rows, :] * f_other[self.first:self.first + n, i:i + 1])
            self.c2.start()

        def merge_across(self):
            n = self.n
            self.mlc[1].wait_recv()
            self.mlc[2].wait_recv()
            tabs = [self.mlbuf[i] for i in range(4)]
            m_pair, m_far = jnp.maximum(tabs[0], tabs[1]), jnp.maximum(tabs[2], tabs[3])
            m_all = jnp.maximum(m_pair, m_far)
            total = jnp.zeros((HL, HD), jnp.float32)
            for t in tabs:
                total = total + jnp.exp(t - m_all) * pltpu.roll(t, HD - B, 1)
            lane = lax.broadcasted_iota(jnp.int32, (HL, HD), 1)
            live = (lane >= self.first) & (lane < self.first + n)
            total = jnp.where(live, total, 1.0)
            g_pair, g_far = columns(jnp.exp(m_pair - m_all) / total), columns(jnp.exp(m_far - m_all) / total)
            self.c2.wait_recv()
            for i in range(half):
                rows = slice(i * n, (i + 1) * n)
                self.oall[self.mine(i), :] = (self.pair[rows, :] * g_pair[self.first:self.first + n, i:i + 1]
                                              + self.r2[rows, :] * g_far[self.first:self.first + n, i:i + 1])
            self.c3.start()

        def project(self):
            n = self.n
            self.c3.wait_recv()
            lhs = [jnp.concatenate([self.oall[2 * i * n:(2 * i + 1) * n, :], self.oall[(2 * i + 1) * n:(2 * i + 2) * n, :]],
                                   axis=1).astype(jnp.bfloat16) for i in range(half)]
            for j in range(NOC):
                y = jnp.zeros((n, OCH), jnp.float32)
                for i in range(half):
                    y = y + jnp.dot(lhs[i], wbuf[i * 2 * HD:(i + 1) * 2 * HD, j * OCH:(j + 1) * OCH],
                                    preferred_element_type=jnp.float32)
                self.ypart[j] = y
                self.pieces[j][0].start()

        def total(self):
            for j in range(NOC):
                self.pieces[j][0].wait_recv()
                self.yall[sp, j] = self.ypart[j] + self.yin[j]
                self.pieces[j][1].start()
                self.pieces[j][2].start()

        def forward(self):
            for j in range(NOC):
                self.pieces[j][1].wait_recv()
                self.pieces[j][3].start()

        def finish(self):
            for j in range(NOC):
                self.pieces[j][2].wait_recv()
                self.pieces[j][3].wait_recv()
            rows = slice(self.first, self.first + self.n)
            for s in range(4):
                for j in range(NOC):
                    at = slice(s * OC + j * OCH, s * OC + (j + 1) * OCH)
                    out_ref[rows, at] = (h_ref[rows, at].astype(jnp.float32) + self.yall[s, j]).astype(jnp.bfloat16)
            for c in (self.c1, self.c2, self.c3, *self.mlc, *(p for ps in self.pieces for p in ps)):
                c.wait_send()

    rest = scratch[2:]
    first = Rows(NA, 0, acc_a, ml_a, rest[:14])
    last = Rows(NB, NA, acc_b, ml_b, rest[14:])
    ml_b[...] = jnp.zeros_like(ml_b)
    pl.semaphore_wait(bar, 4)
    first.start()

    pcol = lax.broadcasted_iota(jnp.int32, (HL, SL), 1)

    def arrive(t):
        for c in reads(t):
            c.wait()

    def score(t):
        sbuf[lax.rem(t, 2)] = scores(g_ref[0, pl.ds(NA + t, HL, stride=B), :], lambda h: kt[t, h])

    def value(t):
        b = NA + t
        at = jnp.full((HL, 1), pos_ref[b] - base)
        here = (at >= 0) & (at < SL)
        q, k_new, v_new = (g_ref[i, pl.ds(b, HL, stride=B), :] for i in range(3))
        s_new = jnp.where(here, jnp.sum(q * k_new, axis=-1, keepdims=True) * SCALE, NEG_BIG)
        valid = pcol < at
        s = jnp.where(valid, sbuf[lax.rem(t, 2)], NEG_BIG)
        m = jnp.maximum(jnp.max(s, axis=-1, keepdims=True), s_new)
        p = jnp.where(valid, jnp.exp(s - m), 0.0)
        p_new = jnp.where(here, jnp.exp(s_new - m), 0.0)
        total = jnp.sum(p, axis=-1, keepdims=True) + p_new
        o = weighted(p, lambda h: vt[t, h]) + p_new.astype(jnp.bfloat16).astype(jnp.float32) * v_new
        acc_b[pl.ds(t, HL, stride=NB), :] = o
        put_stats(ml_b, b, m, total)

    arrive(0)
    score(0)

    @pl.loop(1, NB)
    def _(t):
        arrive(t)
        score(t)
        value(t - 1)

        @pl.when(t == 2)
        def _():
            first.merge_core()

        @pl.when(t == 6)
        def _():
            first.merge_across()

    value(NB - 1)
    last.start()
    for c in wcopies:
        c.wait()
    first.project()
    last.merge_core()
    last.merge_across()
    first.total()
    last.project()
    first.forward()
    last.total()
    first.finish()
    last.forward()
    last.finish()


def write_kernel(pos_ref, g_ref, kin, vin, koin, voin, ko_ref, vo_ref, kt, vt, wsem):
    del kin, vin, koin, voin
    base = lax.axis_index("sp") * SL

    def writes(t):
        return (pltpu.make_async_copy(kt.at[t], ko_ref.at[NA + t], wsem.at[0, t]),
                pltpu.make_async_copy(vt.at[t], vo_ref.at[NA + t], wsem.at[1, t]))

    @pl.loop(0, NB)
    def _(t):
        insert_row(g_ref, NA + t, pos_ref[NA + t] - base, ((1, kt, t), (2, vt, t)))
        for c in writes(t):
            c.start()

    @pl.loop(0, NB)
    def _(t):
        for c in writes(t):
            c.wait()


def solution(mesh):
    half_dim = HD // 2
    freq = 1.0 / (ROPE_BASE ** (np.arange(half_dim, dtype=np.float64) * 2.0 / HD))
    freq = np.concatenate([freq, freq]).astype(np.float32)[None, :]
    f32, bf16 = jnp.float32, jnp.bfloat16
    dma = pltpu.SemaphoreType.DMA

    def shape(dims, dtype):
        return jax.ShapeDtypeStruct(dims, dtype)

    def exchange(n):
        hr = HL // 2 * n
        return [pltpu.VMEM((4, HL, HD), f32), pltpu.VMEM((hr, HD), f32), pltpu.VMEM((hr, HD), f32), pltpu.VMEM((hr, HD), f32),
                pltpu.VMEM((2 * hr, HD), f32), pltpu.VMEM((NOC, n, OCH), f32), pltpu.VMEM((NOC, n, OCH), f32),
                pltpu.VMEM((4, NOC, n, OCH), f32), dma((3,)), dma((3,)), dma((3,)), dma((3,)), dma((4, NOC)), dma((4, NOC))]

    def local_step(hidden, norm_gain, w_query, w_key, w_value, w_out, k_cache, v_cache, positions):
        kt = jnp.transpose(k_cache, (0, 2, 1, 3))
        vt = jnp.transpose(v_cache, (0, 2, 1, 3))
        ring = pltpu.VMEM((SLOTS, HL, SL, HD), bf16)
        g, kring, vring = pl.pallas_call(
            qkv_kernel,
            out_shape=(shape((3, HL * B, HD), f32), ring, ring),
            in_specs=[HBM] * 9,
            out_specs=(VMEM, VMEM, VMEM),
            scratch_shapes=[pltpu.VMEM((3, D, CW), bf16), pltpu.VMEM((B, D), bf16), pltpu.VMEM((3, HL * B, HD), f32),
                            pltpu.SMEM((B,), jnp.int32), pltpu.VMEM((B, D), bf16), pltpu.VMEM((1, D), f32),
                            pltpu.VMEM((1, HD), f32), dma((4,)), dma((3, NKC)), dma((3, 3)), dma((3, 3)), dma((2, EARLY))],
            compiler_params=pltpu.CompilerParams(collective_id=0, has_side_effects=True, vmem_limit_bytes=26 << 20),
            name="qkv",
        )(*(pltpu.with_memory_space_constraint(x, pltpu.HBM) for x in (
            positions, hidden, norm_gain[None, :], jnp.asarray(freq), w_query, w_key, w_value, kt, vt)))

        ko, vo, acc, ml, _, _ = pl.pallas_call(
            cache_kernel,
            out_shape=(shape(kt.shape, bf16), shape(vt.shape, bf16), shape((HL * NA, HD), f32), shape((HL, HD), f32), ring, ring),
            in_specs=[SMEM, VMEM, HBM, HBM, VMEM, VMEM],
            out_specs=(HBM, HBM, VMEM, VMEM, VMEM, VMEM),
            scratch_shapes=[pltpu.VMEM((2, HL, SL), f32), dma((2, SLOTS)), dma((2, SLOTS))],
            input_output_aliases={4: 4, 5: 5},
            compiler_params=pltpu.CompilerParams(vmem_limit_bytes=8 << 20),
            name="cache",
        )(positions, g, kt, vt, kring, vring)

        tiles = pltpu.VMEM((NB, HL, SL, HD), bf16)
        out, kl, vl = pl.pallas_call(
            tail_kernel,
            out_shape=(shape((B, D), bf16), tiles, tiles),
            in_specs=[SMEM, VMEM, VMEM, VMEM, VMEM, HBM, HBM, HBM],
            out_specs=(VMEM, VMEM, VMEM),
            scratch_shapes=[pltpu.VMEM((HL * HD, OC), bf16), pltpu.VMEM((2, HL, SL), f32),
                            pltpu.VMEM((HL * NB, HD), f32), pltpu.VMEM((HL, HD), f32),
                            dma((2, NB)), dma((HL * HD // OK,)), *exchange(NA), *exchange(NB)],
            compiler_params=pltpu.CompilerParams(collective_id=1, has_side_effects=True, vmem_limit_bytes=18 << 20),
            name="tail",
        )(positions, g, acc, ml, hidden, kt, vt, w_out)

        ko, vo, _, _ = pl.pallas_call(
            write_kernel,
            out_shape=(shape(kt.shape, bf16), shape(vt.shape, bf16), tiles, tiles),
            in_specs=[SMEM, VMEM, VMEM, VMEM, HBM, HBM],
            out_specs=(HBM, HBM, VMEM, VMEM),
            scratch_shapes=[dma((2, NB))],
            input_output_aliases={2: 2, 3: 3, 4: 0, 5: 1},
            compiler_params=pltpu.CompilerParams(vmem_limit_bytes=8 << 20),
            name="write",
        )(positions, g, kl, vl, ko, vo)
        return out, jnp.transpose(ko, (0, 2, 1, 3)), jnp.transpose(vo, (0, 2, 1, 3))

    cache_spec = P("dp", "sp", "tp", None)
    specs_in = (P("dp", None), P(None), P(None, "tp"), P(None, "tp"), P(None, "tp"), P("tp", None), cache_spec, cache_spec, P("dp"))
    specs_out = (P("dp", None), cache_spec, cache_spec)
    return jax.shard_map(local_step, mesh=mesh, in_specs=specs_in, out_specs=specs_out, check_vma=False)
```

```python
import jax
import jax.numpy as jnp
import numpy as np
from jax import lax
from jax.experimental import pallas as pl
from jax.experimental.pallas import tpu as pltpu
from jax.sharding import PartitionSpec as P

ROPE_BASE = 1000000.0
EPS = 1e-5
NEG_BIG = -1e30
MESH = pl.DeviceIdType.MESH
VMEM = pl.BlockSpec(memory_space=pltpu.VMEM)
SMEM = pl.BlockSpec(memory_space=pltpu.SMEM)

B = 32
D = 5120
HL = 20
HD = 128
SL = 256
HS = 5
CW = HS * HD
KC = 1280
NKC = D // KC
OC = 1280
OCH = 256
NOC = OC // OCH
OK = 512
GR = 16
NG = B // GR
SLOTS = 9
EARLY = 8
AHEAD = 5
WINDOW = 5
SCALE = HD ** -0.5
HBM = pl.BlockSpec(memory_space=pltpu.HBM)


def peers():
    sp = lax.axis_index("sp")
    across = lax.rem(sp + 2, 4)
    core = sp + 1 - 2 * lax.rem(sp, 2)
    return sp, across, core


def remote(src, dst, send, recv, dev):
    return pltpu.make_async_remote_copy(src_ref=src, dst_ref=dst, send_sem=send, recv_sem=recv,
                                        device_id=dev, device_id_type=MESH)


def qkv_kernel(pos_hbm, h_hbm, gain_hbm, freq_hbm, wq_ref, wk_ref, wv_ref, k_ref, v_ref, out_ref, kring, vring,
               wbuf, xn, g, pos_ref, h_ref, gain_ref, freq_ref, insem, wsem, ssem, rsem, tsem):
    sp, across, core = peers()
    bar = pltpu.get_barrier_semaphore()
    for dev in (across, core):
        pl.semaphore_signal(bar, inc=1, device_id={"sp": dev}, device_id_type=MESH)
    cols = pl.ds(pl.multiple_of(sp * CW, HD), CW)
    small = [pltpu.make_async_copy(src, dst, insem.at[i]) for i, (src, dst) in enumerate(
        ((h_hbm, h_ref), (gain_hbm, gain_ref), (freq_hbm, freq_ref), (pos_hbm, pos_ref)))]
    for c in small:
        c.start()

    def chunk(kind, c):
        src = (wq_ref, wk_ref, wv_ref)[kind]
        rows = pl.ds(c * KC, KC)
        return pltpu.make_async_copy(src.at[rows, cols], wbuf.at[kind, rows], wsem.at[kind, c])

    chunks = [chunk(kind, c) for kind in range(3) for c in range(NKC)]
    tiles = [pltpu.make_async_copy(src.at[b], dst.at[b], tsem.at[i, b])
             for b in range(EARLY) for i, (src, dst) in enumerate(((k_ref, kring), (v_ref, vring)))]
    queue = chunks + tiles
    for c in queue[:WINDOW]:
        c.start()

    for c in small:
        c.wait()
    x = h_ref[...].astype(jnp.float32)
    inv = lax.rsqrt(jnp.mean(x * x, axis=-1, keepdims=True) + EPS)
    xn[...] = (x * inv * gain_ref[...]).astype(jnp.bfloat16)
    row = lax.broadcasted_iota(jnp.int32, (B, HD), 0)
    lane = lax.broadcasted_iota(jnp.int32, (B, HD), 1)
    pos = jnp.zeros((B, HD), jnp.int32)
    for b in range(B):
        pos = jnp.where(row == b, pos_ref[b], pos)
    angles = pos.astype(jnp.float32) * freq_ref[...]
    cosine = jnp.cos(angles)
    sine = jnp.sin(angles)
    sine = jnp.where(lane < HD // 2, -sine, sine)
    pl.semaphore_wait(bar, 2)

    own = pl.ds(pl.multiple_of(sp * HS * B, B), HS * B)
    far = pl.ds(pl.multiple_of(across * HS * B, B), HS * B)
    links = [(remote(g.at[kind, own], g.at[kind, own], ssem.at[kind, 0], rsem.at[kind, 0], {"sp": across}),
              remote(g.at[kind, own], g.at[kind, own], ssem.at[kind, 1], rsem.at[kind, 1], {"sp": core}),
              remote(g.at[kind, far], g.at[kind, far], ssem.at[kind, 2], rsem.at[kind, 2], {"sp": core}))
             for kind in range(3)]

    for kind in range(3):
        acc = jnp.zeros((B, CW), jnp.float32)
        for c in range(NKC):
            step = kind * NKC + c
            chunks[step].wait()
            queue[step + WINDOW].start()
            rows = slice(c * KC, (c + 1) * KC)
            acc = acc + jnp.dot(xn[:, rows], wbuf[kind, rows, :], preferred_element_type=jnp.float32)
        for i in range(HS):
            u = acc[:, i * HD:(i + 1) * HD]
            if kind < 2:
                u = u * cosine + pltpu.roll(u, HD // 2, 1) * sine
            g[kind, pl.ds(pl.multiple_of(sp * HS * B + i * B, B), B), :] = u.astype(jnp.bfloat16).astype(jnp.float32)
        links[kind][0].start()
        links[kind][1].start()
        if kind > 0:
            links[kind - 1][0].wait_recv()
            links[kind - 1][2].start()
    for c in queue[len(chunks) + WINDOW:]:
        c.start()
    links[2][0].wait_recv()
    links[2][2].start()
    for kind in range(3):
        links[kind][0].wait_send()
        links[kind][1].wait()
        links[kind][2].wait()
    out_ref[...] = g[...]
    for c in tiles:
        c.wait()


def row_of(rows, h, x):
    return jnp.where(rows == h, x, 0.0).astype(jnp.bfloat16)


def scores(q, keys):
    rows = lax.broadcasted_iota(jnp.int32, (HL, HD), 0)
    s = jnp.zeros((HL, SL), jnp.float32)
    for h in range(HL):
        s = s + lax.dot_general(row_of(rows, h, q), keys(h), (((1,), (1,)), ((), ())), preferred_element_type=jnp.float32)
    return s * SCALE


def weighted(p, values):
    rows = lax.broadcasted_iota(jnp.int32, (HL, SL), 0)
    o = jnp.zeros((HL, HD), jnp.float32)
    for h in range(HL):
        o = o + jnp.dot(row_of(rows, h, p), values(h), preferred_element_type=jnp.float32)
    return o


def insert_row(g_ref, b, at, tile_refs):
    @pl.when((at >= 0) & (at < SL))
    def _():
        start = pl.multiple_of((at // 16) * 16, 16)
        hit = lax.broadcasted_iota(jnp.int32, (16, HD), 0) == at - start
        for kind, buf, slot in tile_refs:
            for h in range(HL):
                new = jnp.broadcast_to(g_ref[kind, pl.ds(h * B + b, 1), :], (16, HD))
                old = buf[slot, h, pl.ds(start, 16), :].astype(jnp.float32)
                buf[slot, h, pl.ds(start, 16), :] = jnp.where(hit, new, old).astype(jnp.bfloat16)


def put_stats(ml_ref, b, m, total):
    lane = lax.broadcasted_iota(jnp.int32, (HL, HD), 1)
    ml_ref[...] = jnp.where(lane == b, m, jnp.where(lane == b + B, total, ml_ref[...]))


def cache_kernel(pos_ref, g_ref, k_ref, v_ref, kin, vin, ko_ref, vo_ref, acc_ref, ml_ref, kbuf, vbuf,
                 sbuf, rsem, wsem):
    del kin, vin
    base = lax.axis_index("sp") * SL

    def reads(b):
        slot = lax.rem(b, SLOTS)
        return (pltpu.make_async_copy(k_ref.at[b], kbuf.at[slot], rsem.at[0, slot]),
                pltpu.make_async_copy(v_ref.at[b], vbuf.at[slot], rsem.at[1, slot]))

    def write_k(b):
        slot = lax.rem(b, SLOTS)
        return pltpu.make_async_copy(kbuf.at[slot], ko_ref.at[b], wsem.at[0, slot])

    def write_v(b):
        slot = lax.rem(b, SLOTS)
        return pltpu.make_async_copy(vbuf.at[slot], vo_ref.at[b], wsem.at[1, slot])

    for b in range(EARLY, SLOTS):
        for c in reads(b):
            c.start()
    ml_ref[...] = jnp.zeros_like(ml_ref)

    def arrive(b):
        @pl.when(b >= EARLY)
        def _():
            for c in reads(b):
                c.wait()
        slot = lax.rem(b, SLOTS)
        insert_row(g_ref, b, pos_ref[b] - base, ((1, kbuf, slot), (2, vbuf, slot)))

    pcol = lax.broadcasted_iota(jnp.int32, (HL, SL), 1)

    def score(b):
        slot = lax.rem(b, SLOTS)
        sbuf[lax.rem(b, 2)] = scores(g_ref[0, pl.ds(b, HL, stride=B), :], lambda h: kbuf[slot, h])

    def value(b):
        slot = lax.rem(b, SLOTS)
        valid = pcol <= pos_ref[b] - base
        s = jnp.where(valid, sbuf[lax.rem(b, 2)], NEG_BIG)
        m = jnp.max(s, axis=-1, keepdims=True)
        p = jnp.where(valid, jnp.exp(s - m), 0.0)
        total = jnp.sum(p, axis=-1, keepdims=True)
        acc_ref[b // GR, pl.ds(lax.rem(b, GR), HL, stride=GR), :] = weighted(p, lambda h: vbuf[slot, h])
        put_stats(ml_ref, b, m, total)

    def ahead(b):
        @pl.when((b + AHEAD >= SLOTS) & (b + AHEAD < B))
        def _():
            write_k(b + AHEAD - SLOTS).wait()
            write_v(b + AHEAD - SLOTS).wait()
            for c in reads(b + AHEAD):
                c.start()

    arrive(0)
    ahead(0)
    score(0)
    write_k(0).start()
    write_v(0).start()

    @pl.loop(1, B)
    def _(b):
        arrive(b)
        ahead(b)
        score(b)
        value(b - 1)
        write_k(b).start()
        write_v(b).start()

    value(B - 1)
    for b in range(B - SLOTS, B):
        write_k(b).wait()
        write_v(b).wait()


def out_kernel(acc_ref, ml_ref, h_ref, w_ref, out_ref,
               wbuf, mlbuf, r1, pair, r2, oall, ypart, yin, yall,
               wsem, mlsend, mlrecv, ssem, rsem, ysend, yrecv):
    sp, across, core = peers()
    diag = 3 - sp
    tp = lax.axis_index("tp")
    c01 = lax.rem(sp, 2)
    half = HL // 2
    hr = half * GR
    bar = pltpu.get_barrier_semaphore()
    for dev in (core, across, diag):
        pl.semaphore_signal(bar, inc=1, device_id={"sp": dev}, device_id_type=MESH)
    pl.semaphore_signal(bar, inc=1, device_id={"tp": 1 - tp}, device_id_type=MESH)
    wcopies = [pltpu.make_async_copy(w_ref.at[pl.ds(i * OK, OK), pl.ds(pl.multiple_of(sp * OC, HD), OC)],
                                     wbuf.at[pl.ds(i * OK, OK)], wsem.at[i]) for i in range(HL * HD // OK)]
    for c in wcopies:
        c.start()
    mlbuf[0] = ml_ref[...]

    mine = pl.ds(pl.multiple_of(c01 * hr, GR), hr)
    theirs = pl.ds(pl.multiple_of((1 - c01) * hr, GR), hr)
    mlc = [remote(mlbuf.at[0], mlbuf.at[i + 1], mlsend.at[i], mlrecv.at[i], {"sp": dev})
           for i, dev in enumerate((core, across, diag))]
    c1 = [remote(acc_ref.at[i, theirs], r1.at[i], ssem.at[0, i], rsem.at[0, i], {"sp": core}) for i in range(NG)]
    c2 = [remote(pair.at[i], r2.at[i], ssem.at[1, i], rsem.at[1, i], {"sp": across}) for i in range(NG)]
    c3 = [remote(oall.at[i, mine], oall.at[i, mine], ssem.at[2, i], rsem.at[2, i], {"sp": core}) for i in range(NG)]

    def piece(i, j):
        ya = yall.at[i]
        ys, yr = ysend.at[i], yrecv.at[i]
        return (remote(ypart.at[i, j], yin.at[i, j], ys.at[0, j], yr.at[0, j], {"tp": 1 - tp}),
                remote(ya.at[sp, j], ya.at[sp, j], ys.at[1, j], yr.at[1, j], {"sp": across}),
                remote(ya.at[sp, j], ya.at[sp, j], ys.at[2, j], yr.at[2, j], {"sp": core}),
                remote(ya.at[across, j], ya.at[across, j], ys.at[3, j], yr.at[3, j], {"sp": core}))

    pieces = [[piece(i, j) for j in range(NOC)] for i in range(NG)]

    def columns(table):
        t = jnp.where(c01 == 0, table[:half], table[half:])
        t = jnp.concatenate([t, jnp.zeros((HD - half, HD), jnp.float32)], axis=0)
        return jnp.transpose(t)

    def rows_of(h):
        return pl.ds(pl.multiple_of((c01 * half + h) * GR, GR), GR)

    pl.semaphore_wait(bar, 4)
    mlc[0].start()
    for c in c1:
        c.start()
    mlc[1].start()
    mlc[2].start()

    mlc[0].wait_recv()
    m_pair = jnp.maximum(mlbuf[0], mlbuf[1])
    f_own, f_other = columns(jnp.exp(mlbuf[0] - m_pair)), columns(jnp.exp(mlbuf[1] - m_pair))
    for i in range(NG):
        c1[i].wait_recv()
        seqs = slice(i * GR, (i + 1) * GR)
        for h in range(half):
            rows = slice(h * GR, (h + 1) * GR)
            pair[i, rows, :] = acc_ref[i, rows_of(h), :] * f_own[seqs, h:h + 1] + r1[i, rows, :] * f_other[seqs, h:h + 1]
        c2[i].start()

    mlc[1].wait_recv()
    mlc[2].wait_recv()
    tabs = [mlbuf[i] for i in range(4)]
    m_far = jnp.maximum(tabs[2], tabs[3])
    m_all = jnp.maximum(m_pair, m_far)
    total = jnp.zeros((HL, HD), jnp.float32)
    for t in tabs:
        total = total + jnp.exp(t - m_all) * pltpu.roll(t, HD - B, 1)
    total = jnp.where(lax.broadcasted_iota(jnp.int32, (HL, HD), 1) < B, total, 1.0)
    g_pair, g_far = columns(jnp.exp(m_pair - m_all) / total), columns(jnp.exp(m_far - m_all) / total)
    for c in wcopies:
        c.wait()

    def merge(i):
        c2[i].wait_recv()
        seqs = slice(i * GR, (i + 1) * GR)
        for h in range(half):
            rows = slice(h * GR, (h + 1) * GR)
            oall[i, rows_of(h), :] = pair[i, rows, :] * g_pair[seqs, h:h + 1] + r2[i, rows, :] * g_far[seqs, h:h + 1]
        c3[i].start()

    def project(i, side, j):
        y = jnp.zeros((GR, OCH), jnp.float32)
        for h in range(0, half, 2):
            at = [pl.ds(pl.multiple_of((side * half + h + k) * GR, GR), GR) for k in range(2)]
            lhs = jnp.concatenate([oall[i, at[0], :], oall[i, at[1], :]], axis=1).astype(jnp.bfloat16)
            rhs = wbuf[pl.ds(pl.multiple_of((side * half + h) * HD, HD), 2 * HD), j * OCH:(j + 1) * OCH]
            y = y + jnp.dot(lhs, rhs, preferred_element_type=jnp.float32)
        return y

    def own_heads(i):
        for j in range(NOC):
            ypart[i, j] = project(i, c01, j)

    def other_heads(i):
        c3[i].wait_recv()
        for j in range(NOC):
            ypart[i, j] += project(i, 1 - c01, j)
            pieces[i][j][0].start()

    merge(0)
    own_heads(0)
    for i in range(1, NG):
        merge(i)
        other_heads(i - 1)
        own_heads(i)
    other_heads(NG - 1)
    for i in range(NG):
        for j in range(NOC):
            pieces[i][j][0].wait_recv()
            yall[i, sp, j] = ypart[i, j] + yin[i, j]
            pieces[i][j][1].start()
            pieces[i][j][2].start()
    for i in range(NG):
        for j in range(NOC):
            pieces[i][j][1].wait_recv()
            pieces[i][j][3].start()
    for i in range(NG):
        for j in range(NOC):
            pieces[i][j][2].wait_recv()
            pieces[i][j][3].wait_recv()
        for s in range(4):
            for j in range(NOC):
                seqs = slice(i * GR, (i + 1) * GR)
                at = slice(s * OC + j * OCH, s * OC + (j + 1) * OCH)
                out_ref[seqs, at] = (h_ref[seqs, at].astype(jnp.float32) + yall[i, s, j]).astype(jnp.bfloat16)
    for c in (*c1, *c2, *c3, *mlc, *(c for group in pieces for copies in group for c in copies)):
        c.wait_send()


def solution(mesh):
    half_dim = HD // 2
    freq = 1.0 / (ROPE_BASE ** (np.arange(half_dim, dtype=np.float64) * 2.0 / HD))
    freq = np.concatenate([freq, freq]).astype(np.float32)[None, :]
    f32, bf16 = jnp.float32, jnp.bfloat16
    dma = pltpu.SemaphoreType.DMA

    def shape(dims, dtype):
        return jax.ShapeDtypeStruct(dims, dtype)

    def local_step(hidden, norm_gain, w_query, w_key, w_value, w_out, k_cache, v_cache, positions):
        kt = jnp.transpose(k_cache, (0, 2, 1, 3))
        vt = jnp.transpose(v_cache, (0, 2, 1, 3))
        ring = pltpu.VMEM((SLOTS, HL, SL, HD), bf16)
        g, kring, vring = pl.pallas_call(
            qkv_kernel,
            out_shape=(shape((3, HL * B, HD), f32), ring, ring),
            in_specs=[HBM] * 9,
            out_specs=(VMEM, VMEM, VMEM),
            scratch_shapes=[pltpu.VMEM((3, D, CW), bf16), pltpu.VMEM((B, D), bf16), pltpu.VMEM((3, HL * B, HD), f32),
                            pltpu.SMEM((B,), jnp.int32), pltpu.VMEM((B, D), bf16), pltpu.VMEM((1, D), f32),
                            pltpu.VMEM((1, HD), f32), dma((4,)), dma((3, NKC)), dma((3, 3)), dma((3, 3)), dma((2, EARLY))],
            compiler_params=pltpu.CompilerParams(collective_id=0, has_side_effects=True, vmem_limit_bytes=26 << 20),
            name="qkv",
        )(*(pltpu.with_memory_space_constraint(x, pltpu.HBM) for x in (
            positions, hidden, norm_gain[None, :], jnp.asarray(freq), w_query, w_key, w_value, kt, vt)))

        ko, vo, acc, ml, _, _ = pl.pallas_call(
            cache_kernel,
            out_shape=(shape(kt.shape, bf16), shape(vt.shape, bf16), shape((NG, HL * GR, HD), f32), shape((HL, HD), f32), ring, ring),
            in_specs=[SMEM, VMEM, HBM, HBM, VMEM, VMEM],
            out_specs=(HBM, HBM, VMEM, VMEM, VMEM, VMEM),
            scratch_shapes=[pltpu.VMEM((2, HL, SL), f32), dma((2, SLOTS)), dma((2, SLOTS))],
            input_output_aliases={4: 4, 5: 5},
            compiler_params=pltpu.CompilerParams(vmem_limit_bytes=8 << 20),
            name="cache",
        )(positions, g, kt, vt, kring, vring)

        hr = HL // 2 * GR
        out = pl.pallas_call(
            out_kernel,
            out_shape=shape((B, D), bf16),
            in_specs=[VMEM, VMEM, VMEM, HBM],
            out_specs=VMEM,
            scratch_shapes=[pltpu.VMEM((HL * HD, OC), bf16), pltpu.VMEM((4, HL, HD), f32),
                            pltpu.VMEM((NG, hr, HD), f32), pltpu.VMEM((NG, hr, HD), f32), pltpu.VMEM((NG, hr, HD), f32),
                            pltpu.VMEM((NG, 2 * hr, HD), f32), pltpu.VMEM((NG, NOC, GR, OCH), f32),
                            pltpu.VMEM((NG, NOC, GR, OCH), f32), pltpu.VMEM((NG, 4, NOC, GR, OCH), f32),
                            dma((HL * HD // OK,)), dma((3,)), dma((3,)), dma((3, NG)), dma((3, NG)),
                            dma((NG, 4, NOC)), dma((NG, 4, NOC))],
            compiler_params=pltpu.CompilerParams(collective_id=1, has_side_effects=True, vmem_limit_bytes=18 << 20),
            name="out",
        )(acc, ml, hidden, pltpu.with_memory_space_constraint(w_out, pltpu.HBM))
        return out, jnp.transpose(ko, (0, 2, 1, 3)), jnp.transpose(vo, (0, 2, 1, 3))

    cache_spec = P("dp", "sp", "tp", None)
    specs_in = (P("dp", None), P(None), P(None, "tp"), P(None, "tp"), P(None, "tp"), P("tp", None), cache_spec, cache_spec, P("dp"))
    specs_out = (P("dp", None), cache_spec, cache_spec)
    return jax.shard_map(local_step, mesh=mesh, in_specs=specs_in, out_specs=specs_out, check_vma=False)
```

```python
import jax
import jax.numpy as jnp
import numpy as np
from jax import lax
from jax.experimental import pallas as pl
from jax.experimental.pallas import tpu as pltpu
from jax.sharding import PartitionSpec as P

ROPE_BASE = 1000000.0
EPS = 1e-5
NEG_BIG = -1e30
MESH = pl.DeviceIdType.MESH
VMEM = pl.BlockSpec(memory_space=pltpu.VMEM)
SMEM = pl.BlockSpec(memory_space=pltpu.SMEM)

B = 32
D = 5120
HL = 20
HD = 128
SL = 256
HS = 5
CW = HS * HD
KC = 1280
NKC = D // KC
OC = 1280
OCH = 640
NOC = OC // OCH
OK = 512
GR = 16
NG = B // GR
SLOTS = 8
EARLY = 8
BURST = 4
LEAD = 3
JOBS = ((0, 0, 5), (1, 0, 5), (2, 0, 5))
WINDOW = 5
SCALE = HD ** -0.5
HBM = pl.BlockSpec(memory_space=pltpu.HBM)


def peers():
    sp = lax.axis_index("sp")
    across = lax.rem(sp + 2, 4)
    core = sp + 1 - 2 * lax.rem(sp, 2)
    return sp, across, core


def remote(src, dst, send, recv, dev):
    return pltpu.make_async_remote_copy(src_ref=src, dst_ref=dst, send_sem=send, recv_sem=recv,
                                        device_id=dev, device_id_type=MESH)


def qkv_kernel(pos_hbm, h_hbm, gain_hbm, freq_hbm, wq_ref, wk_ref, wv_ref, k_ref, v_ref, out_ref, kring, vring,
               wbuf, xn, g, pos_ref, h_ref, gain_ref, freq_ref, insem, wsem, ssem, rsem, tsem):
    sp, across, core = peers()
    bar = pltpu.get_barrier_semaphore()
    for dev in (across, core):
        pl.semaphore_signal(bar, inc=1, device_id={"sp": dev}, device_id_type=MESH)
    small = [pltpu.make_async_copy(src, dst, insem.at[i]) for i, (src, dst) in enumerate(
        ((h_hbm, h_ref), (gain_hbm, gain_ref), (freq_hbm, freq_ref), (pos_hbm, pos_ref)))]
    for c in small:
        c.start()

    def chunk(job, c):
        kind, first, heads = JOBS[job]
        src = (wq_ref, wk_ref, wv_ref)[kind]
        rows = pl.ds(c * KC, KC)
        cols = pl.ds(pl.multiple_of(sp * CW + first * HD, HD), heads * HD)
        return pltpu.make_async_copy(src.at[rows, cols], wbuf.at[kind, rows, first * HD:(first + heads) * HD], wsem.at[job, c])

    chunks = [chunk(job, c) for job in range(len(JOBS)) for c in range(NKC)]
    tiles = [pltpu.make_async_copy(src.at[b], dst.at[b], tsem.at[i, b])
             for b in range(EARLY) for i, (src, dst) in enumerate(((k_ref, kring), (v_ref, vring)))]
    queue = chunks + tiles
    for c in queue[:WINDOW]:
        c.start()

    for c in small:
        c.wait()
    x = h_ref[...].astype(jnp.float32)
    inv = lax.rsqrt(jnp.mean(x * x, axis=-1, keepdims=True) + EPS)
    xn[...] = (x * inv * gain_ref[...]).astype(jnp.bfloat16)
    row = lax.broadcasted_iota(jnp.int32, (B, HD), 0)
    lane = lax.broadcasted_iota(jnp.int32, (B, HD), 1)
    pos = jnp.zeros((B, HD), jnp.int32)
    for b in range(B):
        pos = jnp.where(row == b, pos_ref[b], pos)
    angles = pos.astype(jnp.float32) * freq_ref[...]
    cosine = jnp.cos(angles)
    sine = jnp.sin(angles)
    sine = jnp.where(lane < HD // 2, -sine, sine)
    pl.semaphore_wait(bar, 2)

    def link(job):
        kind, first, heads = JOBS[job]
        own, far = (g.at[kind, pl.ds(pl.multiple_of(dev * HS * B + first * B, B), heads * B)] for dev in (sp, across))
        return [remote(ref, ref, ssem.at[job, i], rsem.at[job, i], {"sp": dev})
                for i, (ref, dev) in enumerate(((own, across), (own, core), (far, core)))]

    links = [link(job) for job in range(len(JOBS))]
    for job, (kind, first, heads) in enumerate(JOBS):
        acc = jnp.zeros((B, heads * HD), jnp.float32)
        for c in range(NKC):
            step = job * NKC + c
            chunks[step].wait()
            queue[step + WINDOW].start()
            rows = slice(c * KC, (c + 1) * KC)
            acc = acc + jnp.dot(xn[:, rows], wbuf[kind, rows, first * HD:(first + heads) * HD],
                                preferred_element_type=jnp.float32)
        for i in range(heads):
            u = acc[:, i * HD:(i + 1) * HD]
            if kind < 2:
                u = u * cosine + pltpu.roll(u, HD // 2, 1) * sine
            at = pl.ds(pl.multiple_of(sp * HS * B + (first + i) * B, B), B)
            g[kind, at, :] = u.astype(jnp.bfloat16).astype(jnp.float32)
        links[job][0].start()
        links[job][1].start()
        if job > 0:
            links[job - 1][0].wait_recv()
            links[job - 1][2].start()
    for c in queue[len(chunks) + WINDOW:]:
        c.start()
    links[-1][0].wait_recv()
    links[-1][2].start()
    for link in links:
        link[0].wait_send()
        link[1].wait()
        link[2].wait()
    out_ref[...] = g[...]
    for c in tiles:
        c.wait()


def row_of(rows, h, x):
    return jnp.where(rows == h, x, 0.0).astype(jnp.bfloat16)


def scores(q, keys):
    rows = lax.broadcasted_iota(jnp.int32, (HL, HD), 0)
    s = jnp.zeros((HL, SL), jnp.float32)
    for h in range(HL):
        s = s + lax.dot_general(row_of(rows, h, q), keys(h), (((1,), (1,)), ((), ())), preferred_element_type=jnp.float32)
    return s * SCALE


def weighted(p, values):
    rows = lax.broadcasted_iota(jnp.int32, (HL, SL), 0)
    o = jnp.zeros((HL, HD), jnp.float32)
    for h in range(HL):
        o = o + jnp.dot(row_of(rows, h, p), values(h), preferred_element_type=jnp.float32)
    return o


def insert_row(g_ref, b, at, tile_refs):
    @pl.when((at >= 0) & (at < SL))
    def _():
        start = pl.multiple_of((at // 16) * 16, 16)
        hit = lax.broadcasted_iota(jnp.int32, (16, HD), 0) == at - start
        for kind, buf, slot in tile_refs:
            for h in range(HL):
                new = jnp.broadcast_to(g_ref[kind, pl.ds(h * B + b, 1), :], (16, HD))
                old = buf[slot, h, pl.ds(start, 16), :].astype(jnp.float32)
                buf[slot, h, pl.ds(start, 16), :] = jnp.where(hit, new, old).astype(jnp.bfloat16)


def put_stats(ml_ref, b, m, total):
    lane = lax.broadcasted_iota(jnp.int32, (HL, HD), 1)
    ml_ref[...] = jnp.where(lane == b, m, jnp.where(lane == b + B, total, ml_ref[...]))


def cache_kernel(pos_ref, g_ref, k_ref, v_ref, kin, vin, ko_ref, vo_ref, acc_ref, ml_ref, kbuf, vbuf,
                 sbuf, rsem, wsem):
    del kin, vin
    base = lax.axis_index("sp") * SL

    def reads(b):
        slot = lax.rem(b, SLOTS)
        return (pltpu.make_async_copy(k_ref.at[b], kbuf.at[slot], rsem.at[0, slot]),
                pltpu.make_async_copy(v_ref.at[b], vbuf.at[slot], rsem.at[1, slot]))

    def write_k(b):
        slot = lax.rem(b, SLOTS)
        return pltpu.make_async_copy(kbuf.at[slot], ko_ref.at[b], wsem.at[0, slot])

    def write_v(b):
        slot = lax.rem(b, SLOTS)
        return pltpu.make_async_copy(vbuf.at[slot], vo_ref.at[b], wsem.at[1, slot])

    ml_ref[...] = jnp.zeros_like(ml_ref)

    def arrive(b):
        slot = lax.rem(b, SLOTS)
        insert_row(g_ref, b, pos_ref[b] - base, ((1, kbuf, slot), (2, vbuf, slot)))

    pcol = lax.broadcasted_iota(jnp.int32, (HL, SL), 1)

    def score(b):
        slot = lax.rem(b, SLOTS)
        sbuf[lax.rem(b, 2)] = scores(g_ref[0, pl.ds(b, HL, stride=B), :], lambda h: kbuf[slot, h])

    def value(b):
        slot = lax.rem(b, SLOTS)
        valid = pcol <= pos_ref[b] - base
        s = jnp.where(valid, sbuf[lax.rem(b, 2)], NEG_BIG)
        m = jnp.max(s, axis=-1, keepdims=True)
        p = jnp.where(valid, jnp.exp(s - m), 0.0)
        total = jnp.sum(p, axis=-1, keepdims=True)
        acc_ref[b // GR, pl.ds(lax.rem(b, GR), HL, stride=GR), :] = weighted(p, lambda h: vbuf[slot, h])
        put_stats(ml_ref, b, m, total)

    def write(b):
        write_k(b).start()
        write_v(b).start()

    def landed(b):
        for c in reads(b):
            c.wait()

    for b in range(BURST):
        arrive(b)
    for b in range(BURST):
        write(b)

    groups = B // BURST

    def refill(b, more):
        write_k(b).wait()
        write_v(b).wait()

        @pl.when(more)
        def _():
            for c in reads(b + SLOTS):
                c.start()

    @pl.loop(0, groups)
    def _(i):
        first = i * BURST
        more = i + 2 < groups
        score(first)
        for b in range(1, BURST):
            score(first + b)
            value(first + b - 1)
            refill(first + b - 1, more)
        value(first + BURST - 1)
        refill(first + BURST - 1, more)

        @pl.when(i + 1 < groups)
        def _():
            @pl.when(i > 0)
            def _():
                for t in range(BURST - LEAD, BURST):
                    landed(first + BURST + t)
            for t in range(BURST):
                arrive(first + BURST + t)

            @pl.when(more)
            def _():
                for t in range(BURST - LEAD):
                    landed(first + 2 * BURST + t)
            for t in range(BURST):
                write(first + BURST + t)


def out_kernel(acc_ref, ml_ref, h_ref, w_ref, out_ref,
               wbuf, mlbuf, r1, pair, r2, oall, ypart, yin, yall,
               wsem, mlsend, mlrecv, ssem, rsem, ysend, yrecv):
    sp, across, core = peers()
    diag = 3 - sp
    tp = lax.axis_index("tp")
    c01 = lax.rem(sp, 2)
    half = HL // 2
    hr = half * GR
    bar = pltpu.get_barrier_semaphore()
    for dev in (core, across, diag):
        pl.semaphore_signal(bar, inc=1, device_id={"sp": dev}, device_id_type=MESH)
    pl.semaphore_signal(bar, inc=1, device_id={"tp": 1 - tp}, device_id_type=MESH)
    wcopies = [pltpu.make_async_copy(w_ref.at[pl.ds(i * OK, OK), pl.ds(pl.multiple_of(sp * OC, HD), OC)],
                                     wbuf.at[pl.ds(i * OK, OK)], wsem.at[i]) for i in range(HL * HD // OK)]
    for c in wcopies:
        c.start()
    mlbuf[0] = ml_ref[...]

    mine = pl.ds(pl.multiple_of(c01 * hr, GR), hr)
    theirs = pl.ds(pl.multiple_of((1 - c01) * hr, GR), hr)
    mlc = [remote(mlbuf.at[0], mlbuf.at[i + 1], mlsend.at[i], mlrecv.at[i], {"sp": dev})
           for i, dev in enumerate((core, across, diag))]
    c1 = [remote(acc_ref.at[i, theirs], r1.at[i], ssem.at[0, i], rsem.at[0, i], {"sp": core}) for i in range(NG)]
    c2 = [remote(pair.at[i], r2.at[i], ssem.at[1, i], rsem.at[1, i], {"sp": across}) for i in range(NG)]
    c3 = [remote(oall.at[i, mine], oall.at[i, mine], ssem.at[2, i], rsem.at[2, i], {"sp": core}) for i in range(NG)]

    def piece(i, j):
        ya = yall.at[i]
        ys, yr = ysend.at[i], yrecv.at[i]
        return (remote(ypart.at[i, j], yin.at[i, j], ys.at[0, j], yr.at[0, j], {"tp": 1 - tp}),
                remote(ya.at[sp, j], ya.at[sp, j], ys.at[1, j], yr.at[1, j], {"sp": across}),
                remote(ya.at[sp, j], ya.at[sp, j], ys.at[2, j], yr.at[2, j], {"sp": core}),
                remote(ya.at[across, j], ya.at[across, j], ys.at[3, j], yr.at[3, j], {"sp": core}))

    pieces = [[piece(i, j) for j in range(NOC)] for i in range(NG)]

    def columns(table):
        t = jnp.where(c01 == 0, table[:half], table[half:])
        t = jnp.concatenate([t, jnp.zeros((HD - half, HD), jnp.float32)], axis=0)
        return jnp.transpose(t)

    def rows_of(h):
        return pl.ds(pl.multiple_of((c01 * half + h) * GR, GR), GR)

    pl.semaphore_wait(bar, 4)
    mlc[0].start()
    for c in c1:
        c.start()
    mlc[1].start()
    mlc[2].start()

    mlc[0].wait_recv()
    m_pair = jnp.maximum(mlbuf[0], mlbuf[1])
    f_own, f_other = columns(jnp.exp(mlbuf[0] - m_pair)), columns(jnp.exp(mlbuf[1] - m_pair))
    for i in range(NG):
        c1[i].wait_recv()
        seqs = slice(i * GR, (i + 1) * GR)
        for h in range(half):
            rows = slice(h * GR, (h + 1) * GR)
            pair[i, rows, :] = acc_ref[i, rows_of(h), :] * f_own[seqs, h:h + 1] + r1[i, rows, :] * f_other[seqs, h:h + 1]
        c2[i].start()

    mlc[1].wait_recv()
    mlc[2].wait_recv()
    tabs = [mlbuf[i] for i in range(4)]
    m_far = jnp.maximum(tabs[2], tabs[3])
    m_all = jnp.maximum(m_pair, m_far)
    total = jnp.zeros((HL, HD), jnp.float32)
    for t in tabs:
        total = total + jnp.exp(t - m_all) * pltpu.roll(t, HD - B, 1)
    total = jnp.where(lax.broadcasted_iota(jnp.int32, (HL, HD), 1) < B, total, 1.0)
    g_pair, g_far = columns(jnp.exp(m_pair - m_all) / total), columns(jnp.exp(m_far - m_all) / total)
    for c in wcopies:
        c.wait()

    def merge(i):
        c2[i].wait_recv()
        seqs = slice(i * GR, (i + 1) * GR)
        for h in range(half):
            rows = slice(h * GR, (h + 1) * GR)
            oall[i, rows_of(h), :] = pair[i, rows, :] * g_pair[seqs, h:h + 1] + r2[i, rows, :] * g_far[seqs, h:h + 1]
        c3[i].start()

    def project(i, side, j):
        y = jnp.zeros((GR, OCH), jnp.float32)
        for h in range(0, half, 2):
            at = [pl.ds(pl.multiple_of((side * half + h + k) * GR, GR), GR) for k in range(2)]
            lhs = jnp.concatenate([oall[i, at[0], :], oall[i, at[1], :]], axis=1).astype(jnp.bfloat16)
            rhs = wbuf[pl.ds(pl.multiple_of((side * half + h) * HD, HD), 2 * HD), j * OCH:(j + 1) * OCH]
            y = y + jnp.dot(lhs, rhs, preferred_element_type=jnp.float32)
        return y

    def own_heads(i):
        for j in range(NOC):
            ypart[i, j] = project(i, c01, j)

    def other_heads(i):
        c3[i].wait_recv()
        for j in range(NOC):
            ypart[i, j] += project(i, 1 - c01, j)
            pieces[i][j][0].start()

    merge(0)
    own_heads(0)
    for i in range(1, NG):
        merge(i)
        other_heads(i - 1)
        own_heads(i)
    other_heads(NG - 1)
    for i in range(NG):
        for j in range(NOC):
            pieces[i][j][0].wait_recv()
            yall[i, sp, j] = ypart[i, j] + yin[i, j]
            pieces[i][j][1].start()
            pieces[i][j][2].start()
    for i in range(NG):
        for j in range(NOC):
            pieces[i][j][1].wait_recv()
            pieces[i][j][3].start()
    for i in range(NG):
        for j in range(NOC):
            pieces[i][j][2].wait_recv()
            pieces[i][j][3].wait_recv()
        for s in range(4):
            for j in range(NOC):
                seqs = slice(i * GR, (i + 1) * GR)
                at = slice(s * OC + j * OCH, s * OC + (j + 1) * OCH)
                out_ref[seqs, at] = (h_ref[seqs, at].astype(jnp.float32) + yall[i, s, j]).astype(jnp.bfloat16)
    for c in (*c1, *c2, *c3, *mlc, *(c for group in pieces for copies in group for c in copies)):
        c.wait_send()


def solution(mesh):
    half_dim = HD // 2
    freq = 1.0 / (ROPE_BASE ** (np.arange(half_dim, dtype=np.float64) * 2.0 / HD))
    freq = np.concatenate([freq, freq]).astype(np.float32)[None, :]
    f32, bf16 = jnp.float32, jnp.bfloat16
    dma = pltpu.SemaphoreType.DMA

    def shape(dims, dtype):
        return jax.ShapeDtypeStruct(dims, dtype)

    def local_step(hidden, norm_gain, w_query, w_key, w_value, w_out, k_cache, v_cache, positions):
        kt = jnp.transpose(k_cache, (0, 2, 1, 3))
        vt = jnp.transpose(v_cache, (0, 2, 1, 3))
        ring = pltpu.VMEM((SLOTS, HL, SL, HD), bf16)
        g, kring, vring = pl.pallas_call(
            qkv_kernel,
            out_shape=(shape((3, HL * B, HD), f32), ring, ring),
            in_specs=[HBM] * 9,
            out_specs=(VMEM, VMEM, VMEM),
            scratch_shapes=[pltpu.VMEM((3, D, CW), bf16), pltpu.VMEM((B, D), bf16), pltpu.VMEM((3, HL * B, HD), f32),
                            pltpu.SMEM((B,), jnp.int32), pltpu.VMEM((B, D), bf16), pltpu.VMEM((1, D), f32),
                            pltpu.VMEM((1, HD), f32), dma((4,)), dma((len(JOBS), NKC)), dma((len(JOBS), 3)), dma((len(JOBS), 3)), dma((2, EARLY))],
            compiler_params=pltpu.CompilerParams(collective_id=0, has_side_effects=True, vmem_limit_bytes=26 << 20),
            name="qkv",
        )(*(pltpu.with_memory_space_constraint(x, pltpu.HBM) for x in (
            positions, hidden, norm_gain[None, :], jnp.asarray(freq), w_query, w_key, w_value, kt, vt)))

        ko, vo, acc, ml, _, _ = pl.pallas_call(
            cache_kernel,
            out_shape=(shape(kt.shape, bf16), shape(vt.shape, bf16), shape((NG, HL * GR, HD), f32), shape((HL, HD), f32), ring, ring),
            in_specs=[SMEM, VMEM, HBM, HBM, VMEM, VMEM],
            out_specs=(HBM, HBM, VMEM, VMEM, VMEM, VMEM),
            scratch_shapes=[pltpu.VMEM((2, HL, SL), f32), dma((2, SLOTS)), dma((2, SLOTS))],
            input_output_aliases={4: 4, 5: 5},
            compiler_params=pltpu.CompilerParams(vmem_limit_bytes=8 << 20),
            name="cache",
        )(positions, g, kt, vt, kring, vring)

        hr = HL // 2 * GR
        out = pl.pallas_call(
            out_kernel,
            out_shape=shape((B, D), bf16),
            in_specs=[VMEM, VMEM, VMEM, HBM],
            out_specs=VMEM,
            scratch_shapes=[pltpu.VMEM((HL * HD, OC), bf16), pltpu.VMEM((4, HL, HD), f32),
                            pltpu.VMEM((NG, hr, HD), f32), pltpu.VMEM((NG, hr, HD), f32), pltpu.VMEM((NG, hr, HD), f32),
                            pltpu.VMEM((NG, 2 * hr, HD), f32), pltpu.VMEM((NG, NOC, GR, OCH), f32),
                            pltpu.VMEM((NG, NOC, GR, OCH), f32), pltpu.VMEM((NG, 4, NOC, GR, OCH), f32),
                            dma((HL * HD // OK,)), dma((3,)), dma((3,)), dma((3, NG)), dma((3, NG)),
                            dma((NG, 4, NOC)), dma((NG, 4, NOC))],
            compiler_params=pltpu.CompilerParams(collective_id=1, has_side_effects=True, vmem_limit_bytes=18 << 20),
            name="out",
        )(acc, ml, hidden, pltpu.with_memory_space_constraint(w_out, pltpu.HBM))
        return out, jnp.transpose(ko, (0, 2, 1, 3)), jnp.transpose(vo, (0, 2, 1, 3))

    cache_spec = P("dp", "sp", "tp", None)
    specs_in = (P("dp", None), P(None), P(None, "tp"), P(None, "tp"), P(None, "tp"), P("tp", None), cache_spec, cache_spec, P("dp"))
    specs_out = (P("dp", None), cache_spec, cache_spec)
    return jax.shard_map(local_step, mesh=mesh, in_specs=specs_in, out_specs=specs_out, check_vma=False)
```
